32 devices in a mesh: row: 4 (over z), col: 8 (over y, x, core).
Axes of the slice: x: 2, y: 2, z: 4, core: 2. Of those that a mesh axis runs over, the one named last changes fastest.
Arguments:
- right_side: float32 [3, 24576], P(None, ('row', 'col'))
- linewidth: float32 [24576], P(('row', 'col')), may hold values from 0.6 to 2.4
- scattering: float32 [24576, 24576], P('row', 'col'), as said below
Outputs:
- solution: float32 [3, 24576], P(None, ('row', 'col'))
- residual: float32 [3, 24576], P(None, ('row', 'col'))
The draws below stay inside these ranges and needn't reach their ends.
Inputs may be any that keep to these rules, and one draw needn't show every extreme that they name: scattering is symmetric.
All inputs are finite; a program needn't handle non-finite values.
Results may differ from the reference program's by a relative error of at most 0.00018.
Values sent between devices are 32-bit elements; how exact they have to be, the bound alone decides.
No kernel may reach another device: no remote copies, remote signals or barrier semaphores. Data moves between devices by JAX's collectives and lax.ppermute only.
A program may use at most 128 MiB of HBM per device.

```python
import math
import jax
import jax.numpy as jnp
from jax import lax

MODES = 24576
COMPONENTS = 3
ITERS = 2


def draw_scattering(key, part):
    base = jax.random.normal(key, (MODES, MODES), jnp.float32)
    return (base + base.T) * (0.2 / math.sqrt(2.0 * MODES))


def draw_right_side(key, part):
    position = jnp.arange(MODES, dtype=jnp.float32) / (MODES - 1)
    values = jax.random.normal(key, (COMPONENTS, MODES), jnp.float32)
    return values * jnp.exp(math.log(3.0) * position)[None, :]


def block_levels(rng, extent, shards, smallest, top_value):
    def one(axis_at, blocks):
        heights = jax.random.uniform(jax.random.fold_in(jax.random.fold_in(rng, 6), axis_at), (blocks,), jnp.float32, smallest / len(shards), top_value / len(shards))
        return jnp.repeat(jnp.exp(heights), extent[axis_at] // blocks).reshape((-1,) + (1,) * (len(extent) - axis_at - 1))

    gain = one(*shards[0])
    for cut in shards[1:]:
        gain = gain * one(*cut)
    return gain


def setup_inputs(seed: int = 0) -> dict:
    splits = jax.random.split(jax.random.key(seed), 4)
    return {
        "right_side": draw_right_side(jax.random.fold_in(splits[3], 71), 0),
        "linewidth": jnp.clip(jnp.exp(math.log(2.4) - 1.3862944 * jax.random.uniform(splits[1], (MODES,), jnp.float32) ** block_levels(splits[1], (MODES,), ((0, 32),), -0.2, 0.2)), 0.6, 2.4),
        "scattering": draw_scattering(jax.random.fold_in(splits[3], 71), 0),
    }


def apply_operator(vectors, linewidth, scattering):
    product = lax.dot_general(vectors, scattering, (((1,), (1,)), ((), ())), precision=lax.Precision.HIGHEST, preferred_element_type=jnp.float32)
    return linewidth[None, :] * vectors + product


def reference(right_side, linewidth, scattering):
    solution = jnp.zeros_like(right_side)
    residual = right_side
    direction = right_side
    norm_now = jnp.sum(residual * residual, axis=1)
    for iteration in range(ITERS):
        image = apply_operator(direction, linewidth, scattering)
        step_size = norm_now / jnp.sum(direction * image, axis=1)
        solution = solution + step_size[:, None] * direction
        residual = residual - step_size[:, None] * image
        norm_next = jnp.sum(residual * residual, axis=1)
        direction = residual + (norm_next / norm_now)[:, None] * direction
        norm_now = norm_next
    return solution, residual
```

```python
import functools

import jax
import jax.numpy as jnp
from jax import lax
from jax.experimental import pallas as pl
from jax.experimental.pallas import tpu as pltpu
from jax.sharding import PartitionSpec as P

LANES = 128
SUB = 8
BL = 128
CH = 256
RHS = 3
FIRST = 3
SECOND = 6
THIRD = 5
SLOTS = 4
AHEAD = 4

HBM = pl.BlockSpec(memory_space=pltpu.HBM)
VMEM = pl.BlockSpec(memory_space=pltpu.VMEM)


def on_chip(x):
    return pltpu.with_memory_space_constraint(x, pltpu.VMEM)


def row_of(chunk, flip, per_block):
    block = lax.bitwise_xor(chunk // per_block, flip)
    return pl.multiple_of((block * per_block + lax.rem(chunk, per_block)) * CH, CH)


def call(kernel, name, out, limit, ins, scratch=(), **kw):
    return pl.pallas_call(
        kernel,
        name=name,
        in_specs=[HBM if space == "hbm" else VMEM for space in ins],
        out_specs=jax.tree.map(lambda _: VMEM, out),
        out_shape=out,
        scratch_shapes=list(scratch),
        compiler_params=pltpu.CompilerParams(vmem_limit_bytes=limit << 20),
        **kw,
    )


def prefetch_kernel(first, count, flip_of, per_block, s_hbm, after, keep, sem):
    flip = flip_of()
    copies = []
    for i in range(count):
        row = row_of(jnp.int32(first + i), flip, per_block)
        copies.append(
            pltpu.make_async_copy(
                s_hbm.at[pl.ds(row, CH)], keep.at[pl.ds(i * CH, CH)], sem.at[i]
            )
        )
        copies[-1].start()
    for c in copies:
        c.wait()


def merge_kernel(a, b, out):
    out[0:4, :] = a[...]
    out[4:8, :] = b[...]


def spread(v, vb, start):
    t = jnp.transpose(v[:, pl.ds(pl.multiple_of(start, BL), BL)])
    for k in range(RHS):
        vb[k] = jnp.broadcast_to(t[:, k : k + 1], (BL, LANES))


def rows_block(src, row, vb, acc, tiles, v, next_vb, next_start):
    half = tiles // 2
    for h in range(0, tiles, half):
        cols = [slice(c * LANES, (c + 1) * LANES) for c in range(h, h + half)]
        a = [[acc[k, :, c] for c in cols] for k in range(RHS)]
        for g in range(BL // SUB):
            b = [vb[k, g * SUB : (g + 1) * SUB, :] for k in range(RHS)]
            for j, c in enumerate(cols):
                t = src[pl.ds(row + g * SUB, SUB), c]
                for k in range(RHS):
                    a[k][j] = a[k][j] + t * b[k]
        for k in range(RHS):
            for j, c in enumerate(cols):
                acc[k, :, c] = a[k][j]
        if h == 0:
            spread(v, next_vb, next_start)


def cols_block(src, row, wb, part, tiles):
    rows = BL // 2
    for h in range(0, BL, rows):
        a = [jnp.zeros((rows, LANES), jnp.float32)] * RHS
        for c in range(tiles):
            t = src[pl.ds(row + h, rows), c * LANES : (c + 1) * LANES]
            for k in range(RHS):
                b = jnp.concatenate([wb[k * tiles + c]] * (rows // SUB), axis=0)
                a[k] = a[k] + t * b
        for k in range(RHS):
            part[k, h : h + rows, :] = a[k]


def cols_finish(part, zs, block, lane):
    for k in range(RHS):
        total = jnp.sum(jnp.transpose(part[k]), axis=0, keepdims=True)
        zs[block, k : k + 1, pl.ds(pl.multiple_of(lane, BL), BL)] = total


def stream(s_hbm, ring, sem, keep, keep_sem, first, kept, total, flip, per_block, visit):
    def kept_copy(i):
        return pltpu.make_async_copy(
            s_hbm.at[pl.ds(row_of(first + i, flip, per_block), CH)],
            keep.at[pl.ds(pl.multiple_of(i * CH, CH), CH)],
            keep_sem.at[i],
        )

    def ring_copy(i):
        slot = lax.rem(i, SLOTS)
        return pltpu.make_async_copy(
            s_hbm.at[pl.ds(row_of(first + kept + i, flip, per_block), CH)],
            ring.at[slot],
            sem.at[slot],
        )

    rest = total - first - kept

    def start():
        for i in range(min(AHEAD, kept)):
            kept_copy(jnp.int32(i)).start()
        for i in range(min(SLOTS, rest, SLOTS if kept == 0 else max(0, AHEAD - kept))):
            ring_copy(jnp.int32(i)).start()

    begun = min(SLOTS, rest, SLOTS if kept == 0 else max(0, AHEAD - kept))

    def run():
        def kept_step(i, _):
            kept_copy(i).wait()

            @pl.when(i + AHEAD < kept)
            def _():
                kept_copy(i + AHEAD).start()

            if rest > 0:
                ahead = i + AHEAD - kept

                @pl.when((ahead >= begun) & (ahead < min(SLOTS, rest)))
                def _():
                    ring_copy(ahead).start()

            visit(keep, i * CH, first + i)
            return 0

        if kept:
            lax.fori_loop(0, kept, kept_step, 0)

        def ring_step(i, _):
            ring_copy(i).wait()
            visit(ring.at[lax.rem(i, SLOTS)], 0, first + kept + i)

            @pl.when(i + SLOTS < rest)
            def _():
                ring_copy(i + SLOTS).start()

            return 0

        if rest:
            lax.fori_loop(0, rest, ring_step, 0)

    return start, run


def rows_kernel(geo, *refs):
    (nb, blocks, own_blocks, tiles, per_block, counts, total, flip_of, off_of) = geo
    n_keep = sum(1 for c in counts[:2] if c)
    s_hbm, *rest = refs
    keeps = rest[:n_keep]
    pieces = rest[n_keep : n_keep + blocks // 2]
    rest = rest[n_keep + blocks // 2 :]
    if counts[2]:
        out, keep, ring, acc, vb0, vb1, v, keep_sem, sem = rest
    else:
        out, ring, acc, vb0, vb1, v, sem = rest
        keep = keep_sem = None
    flip = flip_of()
    first = counts[0] + counts[1]

    def visit(src, row, chunk):
        at = chunk * CH
        rows_block(src, row, vb0, acc, tiles, v, vb1, at + BL)
        following = jnp.minimum(at + CH, (total - 1) * CH)
        rows_block(src, row + BL, vb1, acc, tiles, v, vb0, following)

    start, run = stream(
        s_hbm, ring, sem, keep, keep_sem, first, counts[2], total, flip, per_block, visit
    )
    start()
    v[4:8, :] = jnp.zeros_like(v[4:8, :])
    for i, piece in enumerate(pieces):
        v[0:4, 2 * i * nb : (2 * i + 1) * nb] = piece[0:4, :]
        v[0:4, (2 * i + 1) * nb : (2 * i + 2) * nb] = piece[4:8, :]
    acc[...] = jnp.zeros_like(acc)
    out[...] = jnp.zeros_like(out)
    spread(v, vb0, jnp.int32(0))
    at = 0
    for ref, count in zip(keeps, [c for c in counts[:2] if c]):

        def step(i, _, ref=ref, at=at):
            visit(ref, i * CH, at + i)
            return 0

        lax.fori_loop(0, count, step, 0)
        at += count
    run()
    for k in range(RHS):
        out[k : k + 1, :] = jnp.sum(acc[k], axis=0, keepdims=True)
    off = off_of()

    @pl.when((off >= 0) & (off < blocks))
    def _():
        for j in range(own_blocks):
            lane = pl.multiple_of(lax.bitwise_xor(off + j, flip) * nb, LANES)
            t = v[:, pl.ds(lane, nb)]
            cols = slice(j * nb, (j + 1) * nb)
            out[0:RHS, cols] = out[0:RHS, cols] + t[3:4] * t[0:RHS]
            out[RHS : 2 * RHS, cols] = t[0:RHS]


def cols_kernel(geo, peers, *refs):
    (nb, blocks, own_blocks, tiles, per_block, counts, total, flip_of, off_of) = geo
    n_keep = sum(1 for c in counts if c)
    s_hbm, *rest = refs
    keeps = rest[:n_keep]
    parts = rest[n_keep : n_keep + peers]
    even, odd, ring, w, wb, p0, p1, zs, sem = rest[n_keep + peers :]
    flip = flip_of()
    first = sum(counts)

    def finish(part, at):
        cols_finish(part, zs, at // nb, lax.rem(at, nb))

    def visit(src, row, chunk):
        at = chunk * CH
        finish(p1, jnp.maximum(at - BL, 0))
        cols_block(src, row, wb, p0, tiles)
        finish(p0, at)
        cols_block(src, row + BL, wb, p1, tiles)

    start, run = stream(
        s_hbm, ring, sem, None, None, first, 0, total, flip, per_block, visit
    )
    start()
    everything = parts[0][...]
    for part in parts[1:]:
        everything = everything + part[...]
    w[...] = everything
    for k in range(RHS):
        for c in range(tiles):
            wb[k * tiles + c] = jnp.broadcast_to(
                w[k : k + 1, c * LANES : (c + 1) * LANES], (SUB, LANES)
            )
    p1[...] = jnp.zeros_like(p1)
    zs[...] = jnp.zeros_like(zs)
    at = 0
    for ref, count in zip(keeps, [c for c in counts if c]):

        def step(i, _, ref=ref, at=at):
            visit(ref, i * CH, at + i)
            return 0

        lax.fori_loop(0, count, step, 0)
        at += count
    run()
    finish(p1, jnp.int32(total * CH - BL))
    off = off_of()

    @pl.when((off >= 0) & (off < blocks))
    def _():
        for j in range(own_blocks):
            at = lax.bitwise_xor(off + j, flip)
            zs[at, RHS : 2 * RHS, :] = w[0:RHS, j * nb : (j + 1) * nb]

    lane = lax.broadcasted_iota(jnp.int32, (1, LANES), 1)
    sums = jnp.zeros((1, LANES), jnp.float32)
    for k in range(RHS):
        b = w[RHS + k : RHS + k + 1, :]
        squares = jnp.sum(b * b, axis=1, keepdims=True)
        products = jnp.sum(b * w[k : k + 1, :], axis=1, keepdims=True)
        sums = sums + jnp.where(lane == k, squares, 0.0)
        sums = sums + jnp.where(lane == RHS + k, products, 0.0)
    for m in range(blocks):
        zs[m, 6:7, 0:LANES] = sums
    for t in range(blocks // 2):
        even[t] = zs[2 * t]
        odd[t] = zs[2 * t + 1]


def add_kernel(a, b, *outs):
    for t, out in enumerate(outs):
        out[...] = a[t] + b[t]


def pick(row, index):
    lane = lax.broadcasted_iota(jnp.int32, row.shape, 1)
    return jnp.sum(jnp.where(lane == index, row, 0.0), axis=1, keepdims=True)


def first_step_kernel(count, *refs):
    parts, (right, width, step, sums) = refs[:count], refs[count:]
    total = parts[0][...]
    for part in parts[1:]:
        total = total + part[...]
    lane = lax.broadcasted_iota(jnp.int32, (1, LANES), 1)
    head = total[6:7, 0:LANES]
    out = jnp.zeros((1, LANES), jnp.float32)
    for k in range(RHS):
        b = right[k : k + 1, :]
        w = total[RHS + k : RHS + k + 1, :]
        z = total[k : k + 1, :] + width[...] * w
        size = pick(head, k) / pick(head, RHS + k)
        residual = b - size * w
        image = w - size * z
        step[k : k + 1, :] = residual
        step[RHS + k : RHS + k + 1, :] = image
        step[8 + k : 9 + k, :] = w
        square = jnp.sum(residual * residual, axis=1, keepdims=True)
        product = jnp.sum(residual * image, axis=1, keepdims=True)
        out = out + jnp.where(lane == k, square, 0.0)
        out = out + jnp.where(lane == RHS + k, product, 0.0)
    step[6:7, :] = total[6:7, :]
    step[7:8, :] = jnp.zeros_like(step[7:8, :])
    step[8 + RHS :, :] = jnp.zeros_like(step[8 + RHS :, :])
    sums[...] = jnp.broadcast_to(out[None], sums.shape)


def second_step_kernel(step, sums, right, solution, residual):
    totals = jnp.sum(sums[...], axis=0)
    head = step[6:7, 0:LANES]
    for k in range(RHS):
        b = right[k : k + 1, :]
        r1 = step[k : k + 1, :]
        image = step[RHS + k : RHS + k + 1, :]
        norm0 = pick(head, k)
        size0 = norm0 / pick(head, RHS + k)
        norm1 = pick(totals, k)
        factor = norm1 / norm0
        size1 = norm1 / (pick(totals, RHS + k) - factor * norm1 / size0)
        w = step[8 + k : 9 + k, :]
        solution[k : k + 1, :] = size0 * b + size1 * (r1 + factor * b)
        residual[k : k + 1, :] = r1 - size1 * (image + factor * w)


def solution(mesh):
    rows, cols = mesh.shape["row"], mesh.shape["col"]
    devices = rows * cols

    def flips(s):
        return [(i, i ^ s) for i in range(cols)]

    def body(right_side, linewidth, scattering):
        n = right_side.shape[1]
        nr, nc = scattering.shape
        fast = n % CH == 0 and cols & (cols - 1) == 0 and cols > 1
        nb = n if fast else nc
        blocks, own_blocks = nr // nb, nc // nb
        tiles = nc // LANES
        total = nr // CH
        per_block = nb // CH

        def flip_of():
            return lax.axis_index("col") if fast else jnp.int32(0)

        def off_of():
            return lax.axis_index("col") * own_blocks - lax.axis_index("row") * blocks

        counts = [FIRST, SECOND, THIRD] if fast else [0, 0, 0]
        f32 = jnp.float32
        shape = jax.ShapeDtypeStruct

        def prefetch(first, count, after):
            return call(
                functools.partial(prefetch_kernel, first, count, flip_of, per_block),
                "prefetch",
                pltpu.VMEM((count * CH, nc), f32),
                1,
                ["hbm", "hbm"],
                [pltpu.SemaphoreType.DMA((count,))],
            )(scattering, after)

        packed = jnp.concatenate([right_side, linewidth[None]], axis=0)
        keeps = []
        if fast:
            other = lax.ppermute(packed, "col", flips(1))
            keeps.append(prefetch(0, counts[0], right_side))
            pair = call(merge_kernel, "merge", shape((8, n), f32), 1, ["", ""])(
                packed, other
            )
            pieces = [pair] + [
                lax.ppermute(pair, "col", flips(s)) for s in range(2, cols, 2)
            ]
            keeps.append(prefetch(counts[0], counts[1], pair))
        else:
            g = lax.all_gather(packed, "col", axis=1, tiled=True)
            g = g.reshape(4, blocks // 2, 2, nb).transpose(1, 2, 0, 3)
            pieces = [g[i].reshape(8, nb) for i in range(blocks // 2)]

        geo = (nb, blocks, own_blocks, tiles, per_block, counts, total, flip_of, off_of)
        scratch = [pltpu.VMEM((SLOTS, CH, nc), f32), pltpu.VMEM((RHS, SUB, nc), f32)]
        scratch += [pltpu.VMEM((RHS, BL, LANES), f32)] * 2 + [pltpu.VMEM((8, nr), f32)]
        out = [shape((8, nc), f32)]
        if counts[2]:
            out.append(pltpu.VMEM((counts[2] * CH, nc), f32))
            scratch.append(pltpu.SemaphoreType.DMA((counts[2],)))
        scratch.append(pltpu.SemaphoreType.DMA((SLOTS,)))
        image, *kept = call(
            functools.partial(rows_kernel, geo),
            "rows_product",
            out,
            20,
            ["hbm"] + [""] * (len(keeps) + len(pieces)),
            scratch,
        )(scattering, *[on_chip(k) for k in keeps], *pieces)
        keeps = keeps + kept
        parts = [image] + [
            lax.ppermute(image, "row", [(i, (i + s) % rows) for i in range(rows)])
            for s in range(1, rows)
        ]
        even, odd = call(
            functools.partial(cols_kernel, geo, len(parts)),
            "cols_product",
            [shape((blocks // 2, 8, nb), f32)] * 2,
            20,
            ["hbm"] + [""] * (len(keeps) + len(parts)),
            [
                pltpu.VMEM((SLOTS, CH, nc), f32),
                pltpu.VMEM((8, nc), f32),
                pltpu.VMEM((RHS * tiles, SUB, LANES), f32),
                pltpu.VMEM((RHS, BL, LANES), f32),
                pltpu.VMEM((RHS, BL, LANES), f32),
                pltpu.VMEM((blocks, 8, nb), f32),
                pltpu.SemaphoreType.DMA((SLOTS,)),
            ],
        )(scattering, *[on_chip(k) for k in keeps], *parts)
        if fast:
            came = lax.ppermute(odd, "col", flips(1))
            sums = call(
                add_kernel,
                "pair_sum",
                [shape((8, n), f32)] * (blocks // 2),
                4,
                ["", ""],
            )(even, came)
            chunks = [sums[0]] + [
                lax.ppermute(sums[t], "col", flips(2 * t)) for t in range(1, blocks // 2)
            ]
        else:
            whole = jnp.stack([even, odd], 1).reshape(blocks, 8, nb)
            heads = lax.psum(whole[0, 6, :LANES], "col")
            whole = whole.transpose(1, 0, 2).reshape(8, nr)
            chunk = lax.psum_scatter(whole, "col", scatter_dimension=1, tiled=True)
            chunks = [chunk.at[6, :LANES].set(heads)]
        step, message = call(
            functools.partial(first_step_kernel, len(chunks)),
            "first_step",
            [shape((16, n), f32), shape((devices, 1, LANES), f32)],
            4,
            [""] * (len(chunks) + 2),
        )(*chunks, right_side, linewidth[None])
        sums = lax.all_to_all(message, ("row", "col"), 0, 0, tiled=True)
        return tuple(
            call(
                second_step_kernel,
                "second_step",
                [shape((RHS, n), f32)] * 2,
                4,
                ["", "", ""],
            )(step, sums, right_side)
        )

    placed = (P(None, ("row", "col")), P(("row", "col")), P("row", "col"))
    return jax.shard_map(
        body,
        mesh=mesh,
        in_specs=placed,
        out_specs=(P(None, ("row", "col")), P(None, ("row", "col"))),
        check_vma=False,
    )
```

```python
import functools

import jax
import jax.numpy as jnp
from jax import lax
from jax.experimental import pallas as pl
from jax.experimental.pallas import tpu as pltpu
from jax.sharding import PartitionSpec as P

LANES = 128
SUB = 8
BL = 128
CH = 256
GROUP = 8
RHS = 3
FIRST = 2
THIRD = 6
STAY = 6
SLOTS = 4
AHEAD = 4
UNROLL = 4
GRANT = 16

HBM = pl.BlockSpec(memory_space=pltpu.HBM)
VMEM = pl.BlockSpec(memory_space=pltpu.VMEM)


def on_chip(x):
    return pltpu.with_memory_space_constraint(x, pltpu.VMEM)


def row_of(chunk, flip, per_block):
    block = lax.bitwise_xor(chunk // per_block, flip)
    return pl.multiple_of((block * per_block + lax.rem(chunk, per_block)) * CH, CH)


def call(kernel, name, out, limit, ins, scratch=(), **kw):
    return pl.pallas_call(
        kernel,
        name=name,
        in_specs=[HBM if space == "hbm" else VMEM for space in ins],
        out_specs=jax.tree.map(lambda _: VMEM, out),
        out_shape=out,
        scratch_shapes=list(scratch),
        compiler_params=pltpu.CompilerParams(vmem_limit_bytes=limit << 20),
        **kw,
    )


def pack_kernel(right, width, out):
    out[0:RHS, :] = right[...]
    out[RHS : RHS + 1, :] = width[...].reshape(1, width.shape[0])


def prefetch_kernel(count, flip_of, per_block, s_hbm, after, keep, sem):
    flip = flip_of()
    copies = []
    for i in range(count):
        row = row_of(jnp.int32(i), flip, per_block)
        copies.append(
            pltpu.make_async_copy(
                s_hbm.at[pl.ds(row, CH)], keep.at[pl.ds(i * CH, CH)], sem.at[i]
            )
        )
        copies[-1].start()
    for c in copies:
        c.wait()


def merge_kernel(a, b, out):
    out[0:4, :] = a[...]
    out[4:8, :] = b[...]


def spread(v, vb, start, rows):
    def one(at):
        t = jnp.transpose(v[:, pl.ds(pl.multiple_of(start + at, BL), BL)])
        for k in range(RHS):
            vb[k, pl.ds(pl.multiple_of(at, BL), BL), :] = jnp.broadcast_to(
                t[:, k : k + 1], (BL, LANES)
            )

    def step(i, _):
        for u in range(UNROLL):
            one(i * (UNROLL * BL) + u * BL)
        return 0

    lax.fori_loop(0, rows // (UNROLL * BL), step, 0)


def rows_block(src, row, vb, at, acc, tiles):
    for h in range(0, tiles, GROUP):
        width = min(GROUP, tiles - h)
        cols = slice(h * LANES, (h + width) * LANES)
        a = [acc[k, :, cols] for k in range(RHS)]
        for g in range(BL // SUB):
            t = src[pl.ds(row + g * SUB, SUB), cols]
            for k in range(RHS):
                b = vb[k, pl.ds(pl.multiple_of(at + g * SUB, SUB), SUB), :]
                a[k] = a[k] + t * jnp.concatenate([b] * width, axis=1)
        for k in range(RHS):
            acc[k, :, cols] = a[k]


def cols_block(src, row, wb, part, tiles):
    rows = BL // 2
    for h in range(0, BL, rows):
        a = [jnp.zeros((rows, LANES), jnp.float32)] * RHS
        for c in range(tiles):
            t = src[pl.ds(row + h, rows), c * LANES : (c + 1) * LANES]
            for k in range(RHS):
                b = jnp.concatenate([wb[k * tiles + c]] * (rows // SUB), axis=0)
                a[k] = a[k] + t * b
        for k in range(RHS):
            part[k, h : h + rows, :] = a[k]


def cols_finish(part, zs, block, lane):
    for k in range(RHS):
        total = jnp.sum(jnp.transpose(part[k]), axis=0, keepdims=True)
        zs[block, k : k + 1, pl.ds(pl.multiple_of(lane, BL), BL)] = total


def stream(s_hbm, ring, sem, keep, keep_sem, first, kept, total, flip, per_block, visit, hi=None):
    def kept_copy(i):
        return pltpu.make_async_copy(
            s_hbm.at[pl.ds(row_of(first + i, flip, per_block), CH)],
            keep.at[pl.ds(pl.multiple_of((first + i) * CH, CH), CH)],
            keep_sem.at[i],
        )

    def ring_copy(i):
        slot = lax.rem(i, SLOTS)
        return pltpu.make_async_copy(
            s_hbm.at[pl.ds(row_of(first + kept + i, flip, per_block), CH)],
            ring.at[slot],
            sem.at[slot],
        )

    rest = total - first - kept

    def start():
        for i in range(min(AHEAD, kept)):
            kept_copy(jnp.int32(i)).start()
        for i in range(min(SLOTS, rest, SLOTS if kept == 0 else max(0, AHEAD - kept))):
            ring_copy(jnp.int32(i)).start()

    begun = min(SLOTS, rest, SLOTS if kept == 0 else max(0, AHEAD - kept))

    def run():
        def kept_step(i, _):
            kept_copy(i).wait()

            @pl.when(i + AHEAD < kept)
            def _():
                kept_copy(i + AHEAD).start()

            if rest > 0:
                ahead = i + AHEAD - kept

                @pl.when((ahead >= begun) & (ahead < min(SLOTS, rest)))
                def _():
                    ring_copy(ahead).start()

            if hi is None or hi >= first + kept:
                visit(keep, (first + i) * CH, first + i)
            else:

                @pl.when(first + i < hi)
                def _():
                    visit(keep, (first + i) * CH, first + i)

            return 0

        if kept:
            lax.fori_loop(0, kept, kept_step, 0)

        def ring_step(i, _):
            ring_copy(i).wait()
            visit(ring.at[lax.rem(i, SLOTS)], 0, first + kept + i)

            @pl.when(i + SLOTS < rest)
            def _():
                ring_copy(i + SLOTS).start()

            return 0

        if rest:
            lax.fori_loop(0, rest, ring_step, 0)

    return start, run


def rows_kernel(geo, lo, hi, have, stay, split, *refs):
    (nb, blocks, own_blocks, tiles, per_block, total, flip_of, off_of) = geo
    s_hbm, *rest = refs
    count = (hi + 2 * per_block - 1) // (2 * per_block)
    pieces, rest = rest[:count], rest[count:]
    before = keep = keep_sem = ring = sem = None
    if lo:
        before, *rest = rest
    if have:
        _, *rest = rest
    out, *rest = rest
    if stay:
        keep, *rest = rest
    if split:
        acc = out
    else:
        acc, *rest = rest
    vb, v, *rest = rest
    if stay:
        keep_sem, *rest = rest
    ringed = max(0, hi - have - stay)
    if ringed:
        ring, sem = rest
    flip = flip_of()
    pair = 2 * nb

    def visit(src, row, chunk):
        at = lax.rem(chunk * CH, pair)

        @pl.when(at == 0)
        def _():
            spread(v, vb, chunk * CH, pair)

        for u in range(0, CH, BL):
            rows_block(src, row + u, vb, at + u, acc, tiles)

    start, run = stream(
        s_hbm, ring, sem, keep, keep_sem, have, stay, have + stay + ringed, flip, per_block, visit, hi
    )
    start()
    v[RHS + 1 :, :] = jnp.zeros_like(v[RHS + 1 :, :])
    for i, piece in enumerate(pieces):
        v[0:4, 2 * i * nb : (2 * i + 1) * nb] = piece[0:4, :]
        v[0:4, (2 * i + 1) * nb : (2 * i + 2) * nb] = piece[4:8, :]
    acc[...] = before[...] if lo else jnp.zeros_like(acc)

    def step(i, _):
        visit(keep, i * CH, i)
        return 0

    if have > lo:
        lax.fori_loop(lo, have, step, 0)
    run()
    if split:
        return
    out[...] = jnp.zeros_like(out)
    for k in range(RHS):
        out[k : k + 1, :] = jnp.sum(acc[k], axis=0, keepdims=True)
    off = off_of()

    @pl.when((off >= 0) & (off < blocks))
    def _():
        for j in range(own_blocks):
            lane = pl.multiple_of(lax.bitwise_xor(off + j, flip) * nb, LANES)
            t = v[:, pl.ds(lane, nb)]
            cols = slice(j * nb, (j + 1) * nb)
            out[0:RHS, cols] = out[0:RHS, cols] + t[3:4] * t[0:RHS]
            out[RHS : 2 * RHS, cols] = t[0:RHS]


def cols_kernel(geo, first, peers, *refs):
    (nb, blocks, own_blocks, tiles, per_block, total, flip_of, off_of) = geo
    s_hbm, *rest = refs
    keep = None
    if first:
        keep, *rest = rest
    parts, rest = rest[:peers], rest[peers:]
    even, odd, ring, w, wb, p0, p1, zs, sem = rest
    flip = flip_of()

    def finish(part, at):
        cols_finish(part, zs, at // nb, lax.rem(at, nb))

    def visit(src, row, chunk):
        at = chunk * CH
        finish(p1, jnp.maximum(at - BL, 0))
        cols_block(src, row, wb, p0, tiles)
        finish(p0, at)
        cols_block(src, row + BL, wb, p1, tiles)

    start, run = stream(
        s_hbm, ring, sem, None, None, first, 0, total, flip, per_block, visit
    )
    start()
    everything = parts[0][...]
    for part in parts[1:]:
        everything = everything + part[...]
    w[...] = everything
    for k in range(RHS):
        for c in range(tiles):
            wb[k * tiles + c] = jnp.broadcast_to(
                w[k : k + 1, c * LANES : (c + 1) * LANES], (SUB, LANES)
            )
    p1[...] = jnp.zeros_like(p1)
    zs[...] = jnp.zeros_like(zs)

    def step(i, _):
        visit(keep, i * CH, i)
        return 0

    if first:
        lax.fori_loop(0, first, step, 0)
    run()
    finish(p1, jnp.int32(total * CH - BL))
    off = off_of()

    @pl.when((off >= 0) & (off < blocks))
    def _():
        for j in range(own_blocks):
            at = lax.bitwise_xor(off + j, flip)
            zs[at, RHS : 2 * RHS, :] = w[0:RHS, j * nb : (j + 1) * nb]

    lane = lax.broadcasted_iota(jnp.int32, (1, LANES), 1)
    sums = jnp.zeros((1, LANES), jnp.float32)
    for k in range(RHS):
        b = w[RHS + k : RHS + k + 1, :]
        squares = jnp.sum(b * b, axis=1, keepdims=True)
        products = jnp.sum(b * w[k : k + 1, :], axis=1, keepdims=True)
        sums = sums + jnp.where(lane == k, squares, 0.0)
        sums = sums + jnp.where(lane == RHS + k, products, 0.0)
    for m in range(blocks):
        zs[m, 6:7, 0:LANES] = sums
    for t in range(blocks // 2):
        even[t] = zs[2 * t]
        odd[t] = zs[2 * t + 1]


def add_kernel(a, b, *outs):
    for t, out in enumerate(outs):
        out[...] = a[t] + b[t]


def pick(row, index):
    lane = lax.broadcasted_iota(jnp.int32, row.shape, 1)
    return jnp.sum(jnp.where(lane == index, row, 0.0), axis=1, keepdims=True)


def first_step_kernel(count, *refs):
    parts, (right, width, step, sums) = refs[:count], refs[count:]
    total = parts[0][...]
    for part in parts[1:]:
        total = total + part[...]
    lane = lax.broadcasted_iota(jnp.int32, (1, LANES), 1)
    head = total[6:7, 0:LANES]
    out = jnp.zeros((1, LANES), jnp.float32)
    for k in range(RHS):
        b = right[k : k + 1, :]
        w = total[RHS + k : RHS + k + 1, :]
        z = total[k : k + 1, :] + width[...] * w
        size = pick(head, k) / pick(head, RHS + k)
        residual = b - size * w
        image = w - size * z
        step[k : k + 1, :] = residual
        step[RHS + k : RHS + k + 1, :] = image
        step[8 + k : 9 + k, :] = w
        square = jnp.sum(residual * residual, axis=1, keepdims=True)
        product = jnp.sum(residual * image, axis=1, keepdims=True)
        out = out + jnp.where(lane == k, square, 0.0)
        out = out + jnp.where(lane == RHS + k, product, 0.0)
    step[6:7, :] = total[6:7, :]
    step[7:8, :] = jnp.zeros_like(step[7:8, :])
    step[8 + RHS :, :] = jnp.zeros_like(step[8 + RHS :, :])
    sums[...] = jnp.broadcast_to(out[None], sums.shape)


def second_step_kernel(step, sums, right, solution, residual):
    totals = jnp.sum(sums[...], axis=0)
    head = step[6:7, 0:LANES]
    for k in range(RHS):
        b = right[k : k + 1, :]
        r1 = step[k : k + 1, :]
        image = step[RHS + k : RHS + k + 1, :]
        norm0 = pick(head, k)
        size0 = norm0 / pick(head, RHS + k)
        norm1 = pick(totals, k)
        factor = norm1 / norm0
        size1 = norm1 / (pick(totals, RHS + k) - factor * norm1 / size0)
        w = step[8 + k : 9 + k, :]
        solution[k : k + 1, :] = size0 * b + size1 * (r1 + factor * b)
        residual[k : k + 1, :] = r1 - size1 * (image + factor * w)


def solution(mesh):
    rows, cols = mesh.shape["row"], mesh.shape["col"]
    devices = rows * cols

    def flips(s):
        return [(i, i ^ s) for i in range(cols)]

    def body(right_side, linewidth, scattering):
        n = right_side.shape[1]
        nr, nc = scattering.shape
        fast = n % CH == 0 and cols & (cols - 1) == 0 and cols > 1
        nb = n if fast else nc
        blocks, own_blocks = nr // nb, nc // nb
        tiles = nc // LANES
        total = nr // CH
        per_block = nb // CH

        def flip_of():
            return lax.axis_index("col") if fast else jnp.int32(0)

        def off_of():
            return lax.axis_index("col") * own_blocks - lax.axis_index("row") * blocks

        f32 = jnp.float32
        shape = jax.ShapeDtypeStruct

        def small(dims):
            return pltpu.VMEM(dims, f32) if fast else shape(dims, f32)

        def near(x):
            return on_chip(x) if fast else x

        kept = pltpu.VMEM(((FIRST + THIRD + STAY) * CH, nc), f32)

        geo = (nb, blocks, own_blocks, tiles, per_block, total, flip_of, off_of)

        def rows_product(lo, hi, have, stay, operands, split, name):
            out = [small((RHS, SUB, nc)) if split else shape((8, nc), f32)]
            scratch = [] if split else [pltpu.VMEM((RHS, SUB, nc), f32)]
            scratch += [pltpu.VMEM((RHS, 2 * nb, LANES), f32), pltpu.VMEM((8, nr), f32)]
            if stay:
                out.append(kept)
                scratch.append(pltpu.SemaphoreType.DMA((stay,)))
            if hi - have - stay > 0:
                scratch.append(pltpu.VMEM((SLOTS, CH, nc), f32))
                scratch.append(pltpu.SemaphoreType.DMA((SLOTS,)))
            return call(
                functools.partial(rows_kernel, geo, lo, hi, have, stay, split),
                name,
                out,
                GRANT,
                ["hbm"] + [""] * len(operands),
                scratch,
                input_output_aliases={len(operands): 1} if have else {},
            )(scattering, *[near(x) for x in operands])

        held = []
        if fast:
            packed = call(pack_kernel, "pack", small((4, n)), GRANT, ["", ""])(
                right_side, linewidth
            )
            other = lax.ppermute(packed, "col", flips(1))
            held = call(
                functools.partial(prefetch_kernel, FIRST, flip_of, per_block),
                "prefetch",
                kept,
                GRANT,
                ["hbm", ""],
                [pltpu.SemaphoreType.DMA((FIRST,))],
            )(scattering, on_chip(packed))
            pair = call(merge_kernel, "merge", small((8, n)), GRANT, ["", ""])(
                on_chip(packed), on_chip(other)
            )
            pieces = [pair] + [
                lax.ppermute(pair, "col", flips(s)) for s in range(2, cols, 2)
            ]
            middle = 2 * per_block
            have = FIRST
            begun, held = rows_product(
                0, middle, have, THIRD, [pair, held], True, "rows_begin"
            )
            have += THIRD
            image, held = rows_product(
                middle, total, have, STAY, pieces + [begun, held], False, "rows_rest"
            )
            have += STAY
            held = [held]
        else:
            packed = jnp.concatenate([right_side, linewidth[None]], axis=0)
            g = lax.all_gather(packed, "col", axis=1, tiled=True)
            g = g.reshape(4, blocks // 2, 2, nb).transpose(1, 2, 0, 3)
            pieces = [g[i].reshape(8, nb) for i in range(blocks // 2)]
            have = 0
            (image,) = rows_product(0, total, 0, 0, pieces, False, "rows_product")
        parts = [image] + [
            lax.ppermute(image, "row", [(i, (i + s) % rows) for i in range(rows)])
            for s in range(1, rows)
        ]
        even, odd = call(
            functools.partial(cols_kernel, geo, have, len(parts)),
            "cols_product",
            [shape((blocks // 2, 8, nb), f32)] * 2,
            GRANT,
            ["hbm"] + [""] * (len(held) + len(parts)),
            [
                pltpu.VMEM((SLOTS, CH, nc), f32),
                pltpu.VMEM((8, nc), f32),
                pltpu.VMEM((RHS * tiles, SUB, LANES), f32),
                pltpu.VMEM((RHS, BL, LANES), f32),
                pltpu.VMEM((RHS, BL, LANES), f32),
                pltpu.VMEM((blocks, 8, nb), f32),
                pltpu.SemaphoreType.DMA((SLOTS,)),
            ],
        )(scattering, *[on_chip(k) for k in held], *parts)
        if fast:
            came = lax.ppermute(odd, "col", flips(1))
            sums = call(
                add_kernel,
                "pair_sum",
                [small((8, n))] * (blocks // 2),
                4,
                ["", ""],
            )(on_chip(even), on_chip(came))
            chunks = [sums[0]] + [
                lax.ppermute(sums[t], "col", flips(2 * t)) for t in range(1, blocks // 2)
            ]
        else:
            whole = jnp.stack([even, odd], 1).reshape(blocks, 8, nb)
            heads = lax.psum(whole[0, 6, :LANES], "col")
            whole = whole.transpose(1, 0, 2).reshape(8, nr)
            chunk = lax.psum_scatter(whole, "col", scatter_dimension=1, tiled=True)
            chunks = [chunk.at[6, :LANES].set(heads)]
        step, message = call(
            functools.partial(first_step_kernel, len(chunks)),
            "first_step",
            [small((16, n)), small((devices, 1, LANES))],
            4,
            [""] * (len(chunks) + 2),
        )(*[near(c) for c in chunks], right_side, linewidth[None])
        sums = lax.all_to_all(message, ("row", "col"), 0, 0, tiled=True)
        return tuple(
            call(
                second_step_kernel,
                "second_step",
                [shape((RHS, n), f32)] * 2,
                4,
                ["", "", ""],
            )(near(step), near(sums), right_side)
        )

    placed = (P(None, ("row", "col")), P(("row", "col")), P("row", "col"))
    return jax.shard_map(
        body,
        mesh=mesh,
        in_specs=placed,
        out_specs=(P(None, ("row", "col")), P(None, ("row", "col"))),
        check_vma=False,
    )
```
